16 devices in a mesh: rep: 1, dp: 16 (over x, y, z, core).
Axes of the slice: x: 2, y: 2, z: 2, core: 2. Of those that a mesh axis runs over, the one named last changes fastest.
Arguments:
- x: bfloat16 [16, 2048, 1280], P(('rep', 'dp'))
- dy: bfloat16 [16, 2048, 1280], P(('rep', 'dp'))
- w_gate: bfloat16 [2, 1280, 3072], replicated
- w_up: bfloat16 [2, 1280, 3072], replicated
- w_down: bfloat16 [2, 3072, 1280], replicated
- m_w_gate: float32 [2, 1280, 3072], P(None, 'dp')
- m_w_up: float32 [2, 1280, 3072], P(None, 'dp')
- m_w_down: float32 [2, 3072, 1280], P(None, 'dp')
- v_w_gate: float32 [2, 1280, 3072], P(None, 'dp')
- v_w_up: float32 [2, 1280, 3072], P(None, 'dp')
- v_w_down: float32 [2, 3072, 1280], P(None, 'dp')
Outputs:
- output 1: bfloat16 [2, 1280, 3072], P('rep')
- output 2: bfloat16 [2, 1280, 3072], P('rep')
- output 3: bfloat16 [2, 3072, 1280], P('rep')
- output 4: float32 [2, 1280, 3072], P('rep', 'dp')
- output 5: float32 [2, 1280, 3072], P('rep', 'dp')
- output 6: float32 [2, 3072, 1280], P('rep', 'dp')
- output 7: float32 [2, 1280, 3072], P('rep', 'dp')
- output 8: float32 [2, 1280, 3072], P('rep', 'dp')
- output 9: float32 [2, 3072, 1280], P('rep', 'dp')
All inputs are finite; a program needn't handle non-finite values.
Results may differ from the reference program's by a relative error of at most 0.022.
Values are sent between devices in bfloat16 or wider.
A program may use at most 2 GiB of HBM per device.

```python
import jax
import jax.numpy as jnp
from jax import lax

SEQUENCES = 16
TOKENS = 2048
D = 1280
FF = 3072
LAYERS = 2
NAMES = ("w_gate", "w_up", "w_down")
SHAPES = {"w_gate": (LAYERS, D, FF), "w_up": (LAYERS, D, FF), "w_down": (LAYERS, FF, D)}


def bump(key, n, height):
    away = (jnp.arange(n, dtype=jnp.int32) - jax.random.randint(key, (), 0, n, jnp.int32)) % n
    return jnp.where(away < n // 8, height, 1.0)


def together(key, own, strength):
    shared = jax.random.normal(key, own.shape[1:], jnp.float32)
    return (own + strength * shared) * lax.rsqrt(1 + strength * strength)


def setup_inputs(seed: int = 0, part: int = 0) -> dict:
    kx, kdy, ka, kb, kz, kf, kh, kl, *keys = jax.random.split(jax.random.key(seed), 8 + 3 * len(NAMES))
    kx, kdy, ka, kb = (jax.random.fold_in(k, part) for k in (kx, kdy, ka, kb))
    kw, km, kv = (keys[i::3] for i in range(3))
    shape = (SEQUENCES, TOKENS, D)
    much_x, much_dy = jax.random.uniform(kz, (2,), jnp.float32, 0.0, 1.0)
    loud = 2.0 ** jax.random.uniform(jax.random.fold_in(kz, 1), (), jnp.float32, -1.0, 2.0)
    layers = 2.0 ** jax.random.uniform(kl, (LAYERS, 1, 1), jnp.float32, -1.0, 1.0)
    x = together(ka, jax.random.normal(kx, shape, jnp.float32), much_x) * bump(kf, D, 4.0)
    dy = together(kb, jax.random.normal(kdy, shape, jnp.float32), much_dy)
    drawn = {"x": x.astype(jnp.bfloat16), "dy": (loud * dy * (SEQUENCES * TOKENS) ** -0.5).astype(jnp.bfloat16)}
    for key, name in zip(kw, NAMES, strict=True):
        w = jax.random.normal(key, SHAPES[name], jnp.float32) * SHAPES[name][1] ** -0.5
        drawn[name] = (w * {"w_gate": 1.0, "w_up": bump(kh, FF, 4.0), "w_down": layers}[name]).astype(jnp.bfloat16)
    for key, name in zip(km, NAMES, strict=True):
        drawn[f"m_{name}"] = 0.1 * jax.random.normal(key, SHAPES[name], jnp.float32)
    for key, name in zip(kv, NAMES, strict=True):
        drawn[f"v_{name}"] = jax.random.uniform(key, SHAPES[name], jnp.float32, 0.005, 0.015)
    return drawn


def matmul(a, w):
    return jnp.dot(a, w, preferred_element_type=jnp.float32).astype(jnp.bfloat16)


def normed(h):
    wide = h.astype(jnp.float32)
    scale = lax.rsqrt(jnp.mean(wide**2, -1, keepdims=True) + 1e-6)
    return (wide * scale).astype(jnp.bfloat16)


def layer(h, w):
    a = normed(h)
    gate = jnp.dot(a, w["w_gate"], preferred_element_type=jnp.float32)
    up = jnp.dot(a, w["w_up"], preferred_element_type=jnp.float32)
    return h + matmul((jax.nn.silu(gate) * up).astype(jnp.bfloat16), w["w_down"])


def adamw(w, m, v, g):
    m = 0.9 * m + 0.1 * g
    v = 0.95 * v + 0.05 * g * g
    step = m * lax.rsqrt(v + 1e-8) + 0.1 * w
    return (w - 0.02 * step).astype(jnp.bfloat16), m, v


def clipped(gradients, sum_of_squares, count):
    factor = jnp.minimum(1.0, 0.5 * lax.rsqrt(sum_of_squares / count + 1e-30))
    return [g * factor for g in gradients]


def stack(weights, h):
    return lax.scan(lambda h, w: (layer(h, w), None), h, weights)[0]


def reference(x, dy, w_gate, w_up, w_down, m_w_gate, m_w_up, m_w_down, v_w_gate, v_w_up, v_w_down):
    weights = dict(zip(NAMES, (w_gate, w_up, w_down), strict=True))

    def take(so_far, sequence):
        h, by_y = sequence
        _, back = jax.vjp(lambda w: stack(w, h), weights)
        return jax.tree.map(lambda total, term: total + term.astype(jnp.float32), so_far, back(by_y)[0]), None

    none_yet = {name: jnp.zeros(w.shape, jnp.float32) for name, w in weights.items()}
    by_weights, _ = lax.scan(take, none_yet, (x, dy))
    gradients = [by_weights[name].astype(jnp.bfloat16).astype(jnp.float32) for name in NAMES]
    gradients = clipped(gradients, sum(jnp.sum(g * g) for g in gradients), sum(g.size for g in gradients))
    new = [
        adamw(w.astype(jnp.float32), m, v, g)
        for w, m, v, g in zip((w_gate, w_up, w_down), (m_w_gate, m_w_up, m_w_down), (v_w_gate, v_w_up, v_w_down), gradients, strict=True)
    ]
    return tuple(one[which] for which in range(3) for one in new)
```

```python
import jax
import jax.numpy as jnp
from jax import lax
from jax.sharding import PartitionSpec as P

F32, BF16 = jnp.float32, jnp.bfloat16


def dot(a, b, contract):
    return lax.dot_general(a, b, ((contract[:1], contract[1:]), ((), ())), preferred_element_type=F32)


def normed(h):
    wide = h.astype(F32)
    scale = lax.rsqrt(jnp.mean(wide**2, -1, keepdims=True) + 1e-6)
    return (wide * scale).astype(BF16), wide, scale


def gated(gate, up):
    return (jax.nn.silu(gate) * up).astype(BF16)


def gated_back(gate, up, d):
    d = d.astype(F32)
    s = jax.nn.sigmoid(gate)
    return (d * up * (s * (1 + gate * (1 - s)))).astype(BF16), (d * (gate * s)).astype(BF16)


def adamw(w, m, v, g):
    m = 0.9 * m + 0.1 * g
    v = 0.95 * v + 0.05 * g * g
    step = m * lax.rsqrt(v + 1e-8) + 0.1 * w
    return (w - 0.02 * step).astype(BF16), m, v


def solution(mesh):
    n = mesh.shape["dp"]

    def step(x, dy, wg, wu, wd, *moments):
        x, dy = x[0], dy[0]
        scatter = lambda g: lax.psum_scatter(g.astype(BF16), "dp", scatter_dimension=0, tiled=True)
        a0, _, _ = normed(x)
        gate0, up0 = dot(a0, wg[0], (1, 0)), dot(a0, wu[0], (1, 0))
        hid0 = gated(gate0, up0)
        h1 = x + dot(hid0, wd[0], (1, 0)).astype(BF16)
        a1, wide1, scale1 = normed(h1)
        gate1, up1 = dot(a1, wg[1], (1, 0)), dot(a1, wu[1], (1, 0))
        hid1 = gated(gate1, up1)
        gd1 = scatter(dot(hid1, dy, (0, 0)))
        dgate1, dup1 = gated_back(gate1, up1, dot(dy, wd[1], (1, 1)).astype(BF16))
        gg1 = scatter(dot(a1, dgate1, (0, 0)))
        gu1 = scatter(dot(a1, dup1, (0, 0)))
        da = dot(dgate1, wg[1], (1, 1)).astype(BF16) + dot(dup1, wu[1], (1, 1)).astype(BF16)
        da = da.astype(F32)
        dwide = scale1 * da - wide1 * (scale1**3 * jnp.mean(da * wide1, -1, keepdims=True))
        dh = dy + dwide.astype(BF16)
        gd0 = scatter(dot(hid0, dh, (0, 0)))
        dgate0, dup0 = gated_back(gate0, up0, dot(dh, wd[0], (1, 1)).astype(BF16))
        gg0 = scatter(dot(a0, dgate0, (0, 0)))
        gu0 = scatter(dot(a0, dup0, (0, 0)))
        grads = [[g.astype(F32) for g in pair] for pair in ((gg0, gg1), (gu0, gu1), (gd0, gd1))]
        total = lax.psum(sum(jnp.sum(g * g) for pair in grads for g in pair), "dp")
        count = wg.size + wu.size + wd.size
        factor = jnp.minimum(1.0, 0.5 * lax.rsqrt(total / count + 1e-30))
        me = lax.axis_index("dp")
        new_w, new_m, new_v = [], [], []
        for w, m, v, pair in zip((wg, wu, wd), moments[:3], moments[3:], grads):
            rows = w.shape[1] // n
            full, ms, vs = [], [], []
            for l in range(2):
                mine = lax.dynamic_slice_in_dim(w[l], me * rows, rows, 0)
                nw, nm, nv = adamw(mine.astype(F32), m[l], v[l], pair[l] * factor)
                full.append(lax.all_gather(nw, "dp", axis=0, tiled=True))
                ms.append(nm)
                vs.append(nv)
            new_w.append(jnp.stack(full))
            new_m.append(jnp.stack(ms))
            new_v.append(jnp.stack(vs))
        return (*new_w, *new_m, *new_v)

    whole, rows = P(None, None, None), P(None, "dp", None)
    outs = (P("rep", None, None),) * 3 + (P("rep", "dp", None),) * 6
    return jax.shard_map(
        step, mesh=mesh, in_specs=(P(("rep", "dp"), None, None),) * 2 + (whole,) * 3 + (rows,) * 6, out_specs=outs, check_vma=False
    )
```

```python
import functools

import jax
import jax.numpy as jnp
from jax import lax
from jax.experimental import pallas as pl
from jax.experimental.pallas import tpu as pltpu
from jax.sharding import PartitionSpec as P

F32, BF16 = jnp.float32, jnp.bfloat16
MESH = pl.DeviceIdType.MESH
BITS = (8, 4, 2)
VMEM_BYTES = 60 * 1024 * 1024
IN_VMEM, IN_HBM = pl.BlockSpec(memory_space=pltpu.VMEM), pl.BlockSpec(memory_space=pl.ANY)


def flip(place, bit):
    return place + bit * (1 - 2 * lax.rem(lax.div(place, bit), 2))


def flips(place, axes, mask):
    for p, axis in enumerate(axes):
        if mask >> p & 1:
            place = flip(place, BITS[axis])
    return place


def meet(places):
    barrier = pltpu.get_barrier_semaphore()
    for place in places:
        pl.semaphore_signal(barrier, inc=1, device_id={"dp": place}, device_id_type=MESH)
    pl.semaphore_wait(barrier, len(places))


def remote(src, dst, send, recv, place):
    return pltpu.make_async_remote_copy(
        src_ref=src, dst_ref=dst, send_sem=send, recv_sem=recv, device_id={"dp": place}, device_id_type=MESH
    )


def turned(turn):
    return tuple((turn + p) % 3 for p in range(3))


def sum_into(dst, terms, rows):
    def body(i, _):
        at = pl.ds(pl.multiple_of(i * 16, 16), 16)
        total = terms[0][at, :].astype(F32)
        for term in terms[1:]:
            total = total + term[at, :].astype(F32)
        dst[at, :] = total.astype(BF16)
        return 0

    lax.fori_loop(0, rows // 16, body, 0)


def scatter_kernel(jobs, *refs):
    grads, outs, rest = refs[:jobs], refs[jobs : 2 * jobs], refs[2 * jobs :]
    own, paired, first, second, third = (rest[k * jobs : (k + 1) * jobs] for k in range(5))
    local_sem, send_pair, recv_pair, send, recv = rest[5 * jobs :]
    me = lax.axis_index("dp")
    core = lax.rem(me, 2)
    partner = flip(me, 1)
    near = [flip(me, bit) for bit in BITS]
    meet([*near, partner])

    order = (1, 3, 5, 7, 2, 6, 4, 0)
    loads, pairs, hops = {}, {}, {}
    for mask in order:
        for j in range(jobs):
            chip = lax.div(flips(me, turned(j), mask), 2)
            pairs[j, mask] = remote(
                grads[j].at[chip, 1 - core], paired[j].at[mask], send_pair.at[j, mask], recv_pair.at[j, mask], partner
            )
            pairs[j, mask].start()
            loads[j, mask] = pltpu.make_async_copy(grads[j].at[chip, core], own[j].at[mask], local_sem.at[j, mask])
            loads[j, mask].start()

    def hop(j, mask, stage):
        dst = (first, second, third)[stage][j].at[mask >> (stage + 1)]
        hops[j, mask] = remote(own[j].at[mask], dst, send.at[j, mask], recv.at[j, mask], near[turned(j)[stage]])
        hops[j, mask].start()

    def add(j, mask, stage):
        loads[j, mask].wait()
        pairs[j, mask].wait_recv()
        terms = [own[j].at[mask], paired[j].at[mask]]
        for s in range(stage):
            hops[j, mask + (1 << s)].wait_recv()
            terms.append((first, second, third)[s][j].at[mask >> (s + 1)])
        sum_into(outs[j] if mask == 0 else own[j].at[mask], terms, own[j].shape[1])

    for stage, masks in enumerate(((1, 3, 5, 7), (2, 6), (4,))):
        for mask in masks:
            for j in range(jobs):
                add(j, mask, stage)
                hop(j, mask, stage)
    for j in range(jobs):
        add(j, 0, 3)
    for copy in (*pairs.values(), *hops.values()):
        copy.wait_send()


def scatter(grads, collective_id):
    jobs = len(grads)
    shapes = [(g.shape[0] // 16, g.shape[1]) for g in grads]
    buffers = lambda n: [pltpu.VMEM((n, *shape), BF16) for shape in shapes]
    sems = pltpu.SemaphoreType.DMA((jobs, 8))
    sent = sum(r * c for r, c in shapes) * 2 * 15
    return pl.pallas_call(
        functools.partial(scatter_kernel, jobs),
        out_shape=[jax.ShapeDtypeStruct(shape, BF16) for shape in shapes],
        in_specs=[IN_HBM] * jobs,
        out_specs=[IN_VMEM] * jobs,
        scratch_shapes=[*buffers(8), *buffers(8), *buffers(4), *buffers(2), *buffers(1), *[sems] * 5],
        compiler_params=pltpu.CompilerParams(collective_id=collective_id, has_side_effects=True, vmem_limit_bytes=VMEM_BYTES),
        cost_estimate=pl.CostEstimate(flops=10**10, bytes_accessed=sent, transcendentals=0),
        name=f"scatter_{collective_id}",
    )(*[g.reshape(8, 2, *shape) for g, shape in zip(grads, shapes)])


def total_kernel(part_ref, out_ref, held, send, recv):
    me = lax.axis_index("dp")
    others = []
    for k in range(1, 16):
        place = me
        for bit in (1, 2, 4, 8):
            if k & bit:
                place = flip(place, bit)
        others.append(place)
    meet(others)
    copies = []
    for k, place in enumerate(others):
        copies.append(remote(part_ref, held.at[k + 1], send.at[k], recv.at[k], place))
        copies[-1].start()
    for copy in copies:
        copy.wait_recv()
    slots = [part_ref[...]] + [held[k] for k in range(1, 16)]
    while len(slots) > 1:
        slots = [slots[i] + slots[i + 1] for i in range(0, len(slots), 2)]
    out_ref[...] = slots[0]
    for copy in copies:
        copy.wait_send()


def total_of(part, collective_id):
    return pl.pallas_call(
        total_kernel,
        out_shape=jax.ShapeDtypeStruct((8, 128), F32),
        in_specs=[IN_VMEM],
        out_specs=IN_VMEM,
        scratch_shapes=[pltpu.VMEM((16, 8, 128), F32), pltpu.SemaphoreType.DMA((15,)), pltpu.SemaphoreType.DMA((15,))],
        compiler_params=pltpu.CompilerParams(collective_id=collective_id, has_side_effects=True),
        name="total",
    )(jnp.full((8, 128), part, F32))[0, 0]


def gather_kernel(count, layers, *refs):
    blocks, outs, rest = refs[:count], refs[count : 2 * count], refs[2 * count :]
    held, (local_sem, send, recv, send_pair, recv_pair) = rest[:count], rest[count:]
    me = lax.axis_index("dp")
    partner = flip(me, 1)
    near = [flip(me, bit) for bit in BITS]
    meet([*near, partner])
    jobs = [(i, l) for l in range(layers) for i in range(count)]

    def slot(i, l, mask):
        return held[i].at[l, mask - 1] if mask else blocks[i].at[l]

    def place_in(i, l, owner):
        rows = blocks[i].shape[1]
        return outs[i].at[l, pl.ds(pl.multiple_of(owner * rows, rows), rows), :]

    hops, pairs, locals_ = {}, {}, {}

    def hop(i, l, mask, stage):
        number = mask + (1 << stage)
        at = (l * count + i, number - 1)
        hops[i, l, number] = remote(slot(i, l, mask), slot(i, l, number), send.at[at], recv.at[at], near[turned(i)[stage]])
        hops[i, l, number].start()

    def hand_on(i, l, mask):
        owner = flips(me, turned(i), mask)
        at = (l * count + i, mask)
        pairs[i, l, mask] = remote(slot(i, l, mask), place_in(i, l, owner), send_pair.at[at], recv_pair.at[at], partner)
        pairs[i, l, mask].start()
        locals_[i, l, mask] = pltpu.make_async_copy(slot(i, l, mask), place_in(i, l, owner), local_sem.at[at])
        locals_[i, l, mask].start()

    for stage in range(3):
        for i, l in jobs:
            hop(i, l, 0, stage)
    for i, l in jobs:
        hand_on(i, l, 0)
    for mask in range(1, 8):
        for i, l in jobs:
            hops[i, l, mask].wait_recv()
            for stage in range(3):
                if mask < 1 << stage:
                    hop(i, l, mask, stage)
            hand_on(i, l, mask)
    for copy in pairs.values():
        copy.wait()
    for copy in hops.values():
        copy.wait_send()
    for copy in locals_.values():
        copy.wait()


def gather(blocks, collective_id):
    count, layers = len(blocks), blocks[0].shape[0]
    shapes = [b.shape[1:] for b in blocks]
    jobs = count * layers
    sent = sum(b.size for b in blocks) * 2 * 15
    return pl.pallas_call(
        functools.partial(gather_kernel, count, layers),
        out_shape=[jax.ShapeDtypeStruct((layers, 16 * r, c), BF16) for r, c in shapes],
        in_specs=[IN_VMEM] * count,
        out_specs=[IN_HBM] * count,
        scratch_shapes=[
            *[pltpu.VMEM((layers, 7, r, c), BF16) for r, c in shapes],
            pltpu.SemaphoreType.DMA((jobs, 8)),
            *[pltpu.SemaphoreType.DMA((jobs, 7))] * 2,
            *[pltpu.SemaphoreType.DMA((jobs, 8))] * 2,
        ],
        compiler_params=pltpu.CompilerParams(collective_id=collective_id, has_side_effects=True, vmem_limit_bytes=VMEM_BYTES),
        cost_estimate=pl.CostEstimate(flops=10**10, bytes_accessed=sent, transcendentals=0),
        name="gather",
    )(*blocks)


def dot(a, b, contract):
    return lax.dot_general(a, b, ((contract[:1], contract[1:]), ((), ())), preferred_element_type=F32)


def normed(h):
    wide = h.astype(F32)
    scale = lax.rsqrt(jnp.mean(wide**2, -1, keepdims=True) + 1e-6)
    return (wide * scale).astype(BF16), wide, scale


def gated(gate, up):
    return (jax.nn.silu(gate) * up).astype(BF16)


def gated_back(gate, up, d):
    d = d.astype(F32)
    s = jax.nn.sigmoid(gate)
    return (d * up * (s * (1 + gate * (1 - s)))).astype(BF16), (d * (gate * s)).astype(BF16)


def adamw(w, m, v, g):
    m = 0.9 * m + 0.1 * g
    v = 0.95 * v + 0.05 * g * g
    step = m * lax.rsqrt(v + 1e-8) + 0.1 * w
    return (w - 0.02 * step).astype(BF16), m, v


def solution(mesh):
    n = mesh.shape["dp"]

    def step(x, dy, wg, wu, wd, *moments):
        x, dy = x[0], dy[0]
        spread = lambda g: lax.psum_scatter(g.astype(BF16), "dp", scatter_dimension=0, tiled=True)
        a0, _, _ = normed(x)
        gate0, up0 = dot(a0, wg[0], (1, 0)), dot(a0, wu[0], (1, 0))
        hid0 = gated(gate0, up0)
        h1 = x + dot(hid0, wd[0], (1, 0)).astype(BF16)
        a1, wide1, scale1 = normed(h1)
        gate1, up1 = dot(a1, wg[1], (1, 0)), dot(a1, wu[1], (1, 0))
        hid1 = gated(gate1, up1)
        gd1 = spread(dot(hid1, dy, (0, 0)))
        dgate1, dup1 = gated_back(gate1, up1, dot(dy, wd[1], (1, 1)).astype(BF16))
        gg1 = spread(dot(a1, dgate1, (0, 0)))
        gu1 = spread(dot(a1, dup1, (0, 0)))
        da = dot(dgate1, wg[1], (1, 1)).astype(BF16) + dot(dup1, wu[1], (1, 1)).astype(BF16)
        da = da.astype(F32)
        dwide = scale1 * da - wide1 * (scale1**3 * jnp.mean(da * wide1, -1, keepdims=True))
        dh = dy + dwide.astype(BF16)
        gd0 = dot(hid0, dh, (0, 0)).astype(BF16)
        dgate0, dup0 = gated_back(gate0, up0, dot(dh, wd[0], (1, 1)).astype(BF16))
        gg0 = dot(a0, dgate0, (0, 0)).astype(BF16)
        gu0 = dot(a0, dup0, (0, 0)).astype(BF16)
        gg0, gu0, gd0 = scatter((gg0, gu0, gd0), 0)
        grads = [[g.astype(F32) for g in pair] for pair in ((gg0, gg1), (gu0, gu1), (gd0, gd1))]
        total = total_of(sum(jnp.sum(g * g) for pair in grads for g in pair), 1)
        count = wg.size + wu.size + wd.size
        factor = jnp.minimum(1.0, 0.5 * lax.rsqrt(total / count + 1e-30))
        me = lax.axis_index("dp")
        new_w, new_m, new_v = [], [], []
        for w, m, v, pair in zip((wg, wu, wd), moments[:3], moments[3:], grads):
            rows = w.shape[1] // n
            mine = lax.dynamic_slice_in_dim(w, me * rows, rows, 1)
            g = jnp.stack(pair) * factor
            for to, value in zip((new_w, new_m, new_v), adamw(mine.astype(F32), m, v, g)):
                to.append(value)
        new_w = gather(new_w, 2)
        return (*new_w, *new_m, *new_v)

    whole, rows = P(None, None, None), P(None, "dp", None)
    outs = (P("rep", None, None),) * 3 + (P("rep", "dp", None),) * 6
    return jax.shard_map(
        step, mesh=mesh, in_specs=(P(("rep", "dp"), None, None),) * 2 + (whole,) * 3 + (rows,) * 6, out_specs=outs, check_vma=False
    )
```

```python
import functools

import jax
import jax.numpy as jnp
from jax import lax
from jax.experimental import pallas as pl
from jax.experimental.pallas import tpu as pltpu
from jax.sharding import PartitionSpec as P

F32, BF16 = jnp.float32, jnp.bfloat16
MESH = pl.DeviceIdType.MESH
BITS = (8, 4, 2)
VMEM_BYTES = 60 * 1024 * 1024
IN_VMEM, IN_HBM = pl.BlockSpec(memory_space=pltpu.VMEM), pl.BlockSpec(memory_space=pl.ANY)


def flip(place, bit):
    return place + bit * (1 - 2 * lax.rem(lax.div(place, bit), 2))


def flips(place, axes, mask):
    for p, axis in enumerate(axes):
        if mask >> p & 1:
            place = flip(place, BITS[axis])
    return place


def meet(places):
    barrier = pltpu.get_barrier_semaphore()
    for place in places:
        pl.semaphore_signal(barrier, inc=1, device_id={"dp": place}, device_id_type=MESH)
    pl.semaphore_wait(barrier, len(places))


def remote(src, dst, send, recv, place):
    return pltpu.make_async_remote_copy(
        src_ref=src, dst_ref=dst, send_sem=send, recv_sem=recv, device_id={"dp": place}, device_id_type=MESH
    )


def turned(turn):
    return tuple((turn + p) % 3 for p in range(3))


def sum_into(dst, terms, rows):
    def body(i, _):
        at = pl.ds(pl.multiple_of(i * 16, 16), 16)
        total = terms[0][at, :].astype(F32)
        for term in terms[1:]:
            total = total + term[at, :].astype(F32)
        dst[at, :] = total.astype(BF16)
        return 0

    lax.fori_loop(0, rows // 16, body, 0)


def scatter_kernel(count, jobs, *refs):
    grads, outs, rest = refs[:count], refs[count : 2 * count], refs[2 * count :]
    n = len(jobs)
    own, paired, first, second, third = (rest[k * n : (k + 1) * n] for k in range(5))
    local_sem, send_pair, recv_pair, send, recv = rest[5 * n :]
    me = lax.axis_index("dp")
    core = lax.rem(me, 2)
    partner = flip(me, 1)
    near = [flip(me, bit) for bit in BITS]
    meet([*near, partner])

    axes = [turned(turn) for _, _, _, turn in jobs]
    loads, pairs, hops = {}, {}, {}
    for mask in (1, 3, 5, 7, 2, 6, 4, 0):
        for j, (i, start, width, _) in enumerate(jobs):
            chip, columns = lax.div(flips(me, axes[j], mask), 2), pl.ds(start, width)
            pairs[j, mask] = remote(
                grads[i].at[chip, 1 - core, :, columns], paired[j].at[mask], send_pair.at[j, mask], recv_pair.at[j, mask], partner
            )
            pairs[j, mask].start()
            loads[j, mask] = pltpu.make_async_copy(grads[i].at[chip, core, :, columns], own[j].at[mask], local_sem.at[j, mask])
            loads[j, mask].start()

    def hop(j, mask, stage):
        dst = (first, second, third)[stage][j].at[mask >> (stage + 1)]
        hops[j, mask] = remote(own[j].at[mask], dst, send.at[j, mask], recv.at[j, mask], near[axes[j][stage]])
        hops[j, mask].start()

    def add(j, mask, stage):
        loads[j, mask].wait()
        pairs[j, mask].wait_recv()
        terms = [own[j].at[mask], paired[j].at[mask]]
        for s in range(stage):
            hops[j, mask + (1 << s)].wait_recv()
            terms.append((first, second, third)[s][j].at[mask >> (s + 1)])
        i, start, width, _ = jobs[j]
        sum_into(outs[i].at[:, pl.ds(start, width)] if mask == 0 else own[j].at[mask], terms, own[j].shape[1])

    for stage, masks in enumerate(((1, 3, 5, 7), (2, 6), (4,))):
        for mask in masks:
            for j in range(n):
                add(j, mask, stage)
                hop(j, mask, stage)
    for j in range(n):
        add(j, 0, 3)
    for copy in (*pairs.values(), *hops.values()):
        copy.wait_send()


def scatter(grads, jobs, collective_id):
    count = len(grads)
    shapes = [(g.shape[0] // 16, g.shape[1]) for g in grads]
    buffers = lambda n: [pltpu.VMEM((n, shapes[i][0], width), BF16) for i, _, width, _ in jobs]
    sems = pltpu.SemaphoreType.DMA((len(jobs), 8))
    sent = sum(r * c for r, c in shapes) * 2 * 15
    return pl.pallas_call(
        functools.partial(scatter_kernel, count, jobs),
        out_shape=[jax.ShapeDtypeStruct(shape, BF16) for shape in shapes],
        in_specs=[IN_HBM] * count,
        out_specs=[IN_VMEM] * count,
        scratch_shapes=[*buffers(8), *buffers(8), *buffers(4), *buffers(2), *buffers(1), *[sems] * 5],
        compiler_params=pltpu.CompilerParams(collective_id=collective_id, has_side_effects=True, vmem_limit_bytes=VMEM_BYTES),
        cost_estimate=pl.CostEstimate(flops=10**10, bytes_accessed=sent, transcendentals=0),
        name=f"scatter_{collective_id}",
    )(*[g.reshape(8, 2, *shape) for g, shape in zip(grads, shapes)])


def total_kernel(count, *refs):
    grads, (out_ref, part_ref, held, send, recv) = refs[:count], refs[count:]
    me = lax.axis_index("dp")
    others = []
    for k in range(1, 16):
        place = me
        for bit in (1, 2, 4, 8):
            if k & bit:
                place = flip(place, bit)
        others.append(place)
    sums = jnp.zeros((8, 128), F32)
    for grad in grads:
        rows, columns = grad.shape

        def body(i, sums, grad=grad, columns=columns):
            g = grad[pl.ds(pl.multiple_of(i * 16, 16), 16), :].astype(F32)
            g = g * g
            g = g[:8] + g[8:]
            tiles = [g[:, c : c + 128] for c in range(0, columns, 128)]
            while len(tiles) > 1:
                tiles = [sum(tiles[c : c + 2]) for c in range(0, len(tiles), 2)]
            return sums + tiles[0]

        sums = lax.fori_loop(0, rows // 16, body, sums)
    part_ref[...] = sums
    meet(others)
    copies = []
    for k, place in enumerate(others):
        copies.append(remote(part_ref, held.at[k], send.at[k], recv.at[k], place))
        copies[-1].start()
    for copy in copies:
        copy.wait_recv()
    slots = [part_ref[...]] + [held[k] for k in range(15)]
    while len(slots) > 1:
        slots = [slots[i] + slots[i + 1] for i in range(0, len(slots), 2)]
    out_ref[...] = jnp.zeros((8, 128), F32) + jnp.sum(slots[0])
    for copy in copies:
        copy.wait_send()


def total_of(grads, collective_id):
    return pl.pallas_call(
        functools.partial(total_kernel, len(grads)),
        out_shape=jax.ShapeDtypeStruct((8, 128), F32),
        in_specs=[IN_VMEM] * len(grads),
        out_specs=IN_VMEM,
        scratch_shapes=[
            pltpu.VMEM((8, 128), F32), pltpu.VMEM((15, 8, 128), F32), pltpu.SemaphoreType.DMA((15,)), pltpu.SemaphoreType.DMA((15,))
        ],
        compiler_params=pltpu.CompilerParams(collective_id=collective_id, has_side_effects=True),
        name="total",
    )(*grads)[0, 0]


def gather_kernel(count, layers, *refs):
    blocks, outs, rest = refs[:count], refs[count : 2 * count], refs[2 * count :]
    held, (local_sem, send, recv, send_pair, recv_pair) = rest[:count], rest[count:]
    me = lax.axis_index("dp")
    partner = flip(me, 1)
    near = [flip(me, bit) for bit in BITS]
    meet([*near, partner])
    jobs = [(i, l) for l in range(layers) for i in range(count)]

    def slot(i, l, mask):
        return held[i].at[l, mask - 1] if mask else blocks[i].at[l]

    def place_in(i, l, owner):
        rows = blocks[i].shape[1]
        return outs[i].at[l, pl.ds(pl.multiple_of(owner * rows, rows), rows), :]

    hops, pairs, locals_ = {}, {}, {}

    def hop(i, l, mask, stage):
        number = mask + (1 << stage)
        at = (l * count + i, number - 1)
        hops[i, l, number] = remote(slot(i, l, mask), slot(i, l, number), send.at[at], recv.at[at], near[turned(i)[stage]])
        hops[i, l, number].start()

    def hand_on(i, l, mask):
        owner = flips(me, turned(i), mask)
        at = (l * count + i, mask)
        pairs[i, l, mask] = remote(slot(i, l, mask), place_in(i, l, owner), send_pair.at[at], recv_pair.at[at], partner)
        pairs[i, l, mask].start()
        locals_[i, l, mask] = pltpu.make_async_copy(slot(i, l, mask), place_in(i, l, owner), local_sem.at[at])
        locals_[i, l, mask].start()

    for stage in range(3):
        for i, l in jobs:
            hop(i, l, 0, stage)
    for i, l in jobs:
        hand_on(i, l, 0)
    for mask in range(1, 8):
        for i, l in jobs:
            hops[i, l, mask].wait_recv()
            for stage in range(3):
                if mask < 1 << stage:
                    hop(i, l, mask, stage)
            hand_on(i, l, mask)
    for copy in pairs.values():
        copy.wait()
    for copy in hops.values():
        copy.wait_send()
    for copy in locals_.values():
        copy.wait()


def gather(blocks, collective_id):
    count, layers = len(blocks), blocks[0].shape[0]
    shapes = [b.shape[1:] for b in blocks]
    jobs = count * layers
    sent = sum(b.size for b in blocks) * 2 * 15
    return pl.pallas_call(
        functools.partial(gather_kernel, count, layers),
        out_shape=[jax.ShapeDtypeStruct((layers, 16 * r, c), BF16) for r, c in shapes],
        in_specs=[IN_VMEM] * count,
        out_specs=[IN_HBM] * count,
        scratch_shapes=[
            *[pltpu.VMEM((layers, 7, r, c), BF16) for r, c in shapes],
            pltpu.SemaphoreType.DMA((jobs, 8)),
            *[pltpu.SemaphoreType.DMA((jobs, 7))] * 2,
            *[pltpu.SemaphoreType.DMA((jobs, 8))] * 2,
        ],
        compiler_params=pltpu.CompilerParams(collective_id=collective_id, has_side_effects=True, vmem_limit_bytes=VMEM_BYTES),
        cost_estimate=pl.CostEstimate(flops=10**10, bytes_accessed=sent, transcendentals=0),
        name="gather",
    )(*blocks)


def dot(a, b, contract):
    return lax.dot_general(a, b, ((contract[:1], contract[1:]), ((), ())), preferred_element_type=F32)


def scale_of(wide):
    return lax.rsqrt(jnp.mean(wide * wide, -1, keepdims=True) + 1e-6)


def normed(h):
    wide = h.astype(F32)
    return (wide * scale_of(wide)).astype(BF16)


def gated_back(gate, up, d):
    s = jax.nn.sigmoid(gate)
    return (d * up * (s * (1 + gate * (1 - s)))).astype(BF16), (d * (gate * s)).astype(BF16)


def run(kernel, name, grid, ins, outs, flops):
    moved = sum(a.size * a.dtype.itemsize for a, _, _ in ins)
    return pl.pallas_call(
        kernel,
        grid=grid,
        in_specs=[pl.BlockSpec(block, index) for _, block, index in ins],
        out_specs=[pl.BlockSpec(block, index) for _, _, block, index in outs],
        out_shape=[jax.ShapeDtypeStruct(shape, kind) for shape, kind, _, _ in outs],
        compiler_params=pltpu.CompilerParams(dimension_semantics=("arbitrary",) * len(grid), vmem_limit_bytes=VMEM_BYTES),
        cost_estimate=pl.CostEstimate(flops=flops, bytes_accessed=moved, transcendentals=0),
        name=name,
    )(*[a for a, _, _ in ins])


def pieces(width, piece):
    return [pl.ds(at, piece) for at in range(0, width, piece)]


def up_kernel(x_ref, wg_ref, wu_ref, a_ref, gate_ref, up_ref, hid_ref):
    @pl.when(pl.program_id(1) == 0)
    def _():
        def body(i, _):
            at = pl.ds(pl.multiple_of(i * 128, 128), 128)
            a_ref[at, :] = normed(x_ref[at, :])
            return 0

        lax.fori_loop(0, x_ref.shape[0] // 128, body, 0)

    for at in pieces(gate_ref.shape[1], 256):
        gate, up = dot(a_ref[...], wg_ref[0, :, at], (1, 0)), dot(a_ref[...], wu_ref[0, :, at], (1, 0))
        gate_ref[:, at] = gate
        up_ref[:, at] = up
        hid_ref[:, at] = (gate * jax.nn.sigmoid(gate) * up).astype(BF16)


def up_layer(x, wg, wu, l):
    (t, d), f = x.shape, wg.shape[2]
    tm, tn = 1024, 512
    row, weight, tile = (lambda i, j: (i, 0)), (lambda i, j: (l, 0, j)), (lambda i, j: (i, j))
    return run(
        up_kernel, "up", (t // tm, f // tn),
        [(x, (tm, d), row), (wg, (1, d, tn), weight), (wu, (1, d, tn), weight)],
        [((t, d), BF16, (tm, d), row), *[((t, f), kind, (tm, tn), tile) for kind in (F32, F32, BF16)]],
        4 * t * d * f,
    )


def down_kernel(hid_ref, w_ref, x_ref, h_ref, a_ref):
    half = hid_ref.shape[0] // 2
    for at in (pl.ds(0, half), pl.ds(half, half)):
        h = x_ref[at, :] + dot(hid_ref[at, :], w_ref[0], (1, 0)).astype(BF16)
        h_ref[at, :] = h
        a_ref[at, :] = normed(h)


def down_layer(hid, wd, x, l):
    (t, f), d = hid.shape, wd.shape[2]
    tm = 512
    row = lambda i: (i, 0)
    return run(
        down_kernel, "down", (t // tm,),
        [(hid, (tm, f), row), (wd, (1, f, d), lambda i: (l, 0, 0)), (x, (tm, d), row)],
        [((t, d), BF16, (tm, d), row)] * 2,
        2 * t * d * f,
    )


def turn_kernel(a_ref, dy_ref, wg_ref, wu_ref, wd_ref, hid_ref, dgate_ref, dup_ref):
    for at in pieces(hid_ref.shape[1], 256):
        gate, up = dot(a_ref[...], wg_ref[0, :, at], (1, 0)), dot(a_ref[...], wu_ref[0, :, at], (1, 0))
        d = dot(dy_ref[...], wd_ref[0, at, :], (1, 1)).astype(BF16).astype(F32)
        hid_ref[:, at] = (gate * jax.nn.sigmoid(gate) * up).astype(BF16)
        dgate_ref[:, at], dup_ref[:, at] = gated_back(gate, up, d)


def turn_layer(a, dy, wg, wu, wd, l):
    (t, d), f = a.shape, wg.shape[2]
    tm, tn = 1024, 512
    row, weight, tile = (lambda i, j: (i, 0)), (lambda i, j: (l, 0, j)), (lambda i, j: (i, j))
    return run(
        turn_kernel, "turn", (t // tm, f // tn),
        [(a, (tm, d), row), (dy, (tm, d), row), *[(w, (1, d, tn), weight) for w in (wg, wu)], (wd, (1, tn, d), lambda i, j: (l, j, 0))],
        [((t, f), BF16, (tm, tn), tile)] * 3,
        6 * t * d * f,
    )


def back_kernel(dgate_ref, dup_ref, wg_ref, wu_ref, h_ref, dy_ref, dh_ref):
    da = dot(dgate_ref[...], wg_ref[0], (1, 1)).astype(BF16) + dot(dup_ref[...], wu_ref[0], (1, 1)).astype(BF16)
    da, wide = da.astype(F32), h_ref[...].astype(F32)
    scale = scale_of(wide)
    dwide = scale * da - wide * (scale * scale * scale * jnp.mean(da * wide, -1, keepdims=True))
    dh_ref[...] = dy_ref[...] + dwide.astype(BF16)


def back_layer(dgate, dup, wg, wu, h, dy, l):
    (t, f), d = dgate.shape, wg.shape[1]
    tm = 512
    row = lambda i: (i, 0)
    return run(
        back_kernel, "back", (t // tm,),
        [*[(g, (tm, f), row) for g in (dgate, dup)], *[(w, (1, d, f), lambda i: (l, 0, 0)) for w in (wg, wu)], (h, (tm, d), row), (dy, (tm, d), row)],
        [((t, d), BF16, (tm, d), row)],
        4 * t * d * f,
    )[0]


def hidden_kernel(dh_ref, wd_ref, gate_ref, up_ref, dgate_ref, dup_ref):
    for at in pieces(gate_ref.shape[1], 256):
        d = dot(dh_ref[...], wd_ref[0, at, :], (1, 1)).astype(BF16).astype(F32)
        dgate_ref[:, at], dup_ref[:, at] = gated_back(gate_ref[:, at], up_ref[:, at], d)


def hidden_back(dh, wd, gate, up, l):
    (t, d), f = dh.shape, gate.shape[1]
    tm, tn = 1024, 512
    row, tile = (lambda i, j: (i, 0)), (lambda i, j: (i, j))
    return run(
        hidden_kernel, "hidden", (t // tm, f // tn),
        [(dh, (tm, d), row), (wd, (1, tn, d), lambda i, j: (l, j, 0)), (gate, (tm, tn), tile), (up, (tm, tn), tile)],
        [((t, f), BF16, (tm, tn), tile)] * 2,
        2 * t * d * f,
    )


def weight_kernel(a_ref, b_ref, out_ref):
    out_ref[...] = dot(a_ref[...], b_ref[...], (0, 0)).astype(BF16)


def weight_grad(a, b):
    (t, p), q = a.shape, b.shape[1]
    tp, tq = (640, 1024) if p < q else (768, 1280)
    return run(
        weight_kernel, "weight", (p // tp, q // tq),
        [(a, (t, tp), lambda i, j: (0, i)), (b, (t, tq), lambda i, j: (0, j))],
        [((p, q), BF16, (tp, tq), lambda i, j: (i, j))],
        2 * t * p * q,
    )[0]


def adamw(w, m, v, g):
    m = 0.9 * m + 0.1 * g
    v = 0.95 * v + 0.05 * g * g
    step = m * lax.rsqrt(v + 1e-8) + 0.1 * w
    return (w - 0.02 * step).astype(BF16), m, v


def solution(mesh):
    n = mesh.shape["dp"]

    def step(x, dy, wg, wu, wd, *moments):
        x, dy = x[0], dy[0]
        spread = lambda g: lax.psum_scatter(g, "dp", scatter_dimension=0, tiled=True)
        a0, gate0, up0, hid0 = up_layer(x, wg, wu, 0)
        h1, a1 = down_layer(hid0, wd, x, 0)
        hid1, dgate1, dup1 = turn_layer(a1, dy, wg, wu, wd, 1)
        gd1 = spread(weight_grad(hid1, dy))
        gg1 = spread(weight_grad(a1, dgate1))
        gu1 = weight_grad(a1, dup1)
        dh = back_layer(dgate1, dup1, wg, wu, h1, dy, 1)
        gd0 = weight_grad(hid0, dh)
        dgate0, dup0 = hidden_back(dh, wd, gate0, up0, 0)
        gg0, gu0 = weight_grad(a0, dgate0), weight_grad(a0, dup0)
        f, d = wg.shape[2], wd.shape[2]
        thirds = [(3, k * (f // 3), f // 3, k) for k in range(3)]
        gg0, gu0, gd0, gu1 = scatter((gg0, gu0, gd0, gu1), (*thirds, (2, 0, d, 2), (0, 0, f, 0), (1, 0, f, 1)), 0)
        grads = ((gg0, gg1), (gu0, gu1), (gd0, gd1))
        total = total_of([g for pair in grads for g in pair], 1)
        count = wg.size + wu.size + wd.size
        factor = jnp.minimum(1.0, 0.5 * lax.rsqrt(total / count + 1e-30))
        me = lax.axis_index("dp")
        new_w, new_m, new_v = [], [], []
        for w, m, v, pair in zip((wg, wu, wd), moments[:3], moments[3:], grads):
            rows = w.shape[1] // n
            mine = lax.dynamic_slice_in_dim(w, me * rows, rows, 1)
            g = jnp.stack(pair).astype(F32) * factor
            for to, value in zip((new_w, new_m, new_v), adamw(mine.astype(F32), m, v, g)):
                to.append(value)
        new_w = gather(new_w, 2)
        return (*new_w, *new_m, *new_v)

    whole, rows = P(None, None, None), P(None, "dp", None)
    outs = (P("rep", None, None),) * 3 + (P("rep", "dp", None),) * 6
    return jax.shard_map(
        step, mesh=mesh, in_specs=(P(("rep", "dp"), None, None),) * 2 + (whole,) * 3 + (rows,) * 6, out_specs=outs, check_vma=False
    )
```

```python
import functools

import jax
import jax.numpy as jnp
from jax import lax
from jax.experimental import pallas as pl
from jax.experimental.pallas import tpu as pltpu
from jax.sharding import PartitionSpec as P

F32, BF16 = jnp.float32, jnp.bfloat16
MESH = pl.DeviceIdType.MESH
BITS = (8, 4, 2)
VMEM_BYTES = 60 * 1024 * 1024
IN_VMEM, IN_HBM = pl.BlockSpec(memory_space=pltpu.VMEM), pl.BlockSpec(memory_space=pl.ANY)


def flip(place, bit):
    return place + bit * (1 - 2 * lax.rem(lax.div(place, bit), 2))


def flips(place, axes, mask):
    for p, axis in enumerate(axes):
        if mask >> p & 1:
            place = flip(place, BITS[axis])
    return place


def meet(places):
    barrier = pltpu.get_barrier_semaphore()
    for place in places:
        pl.semaphore_signal(barrier, inc=1, device_id={"dp": place}, device_id_type=MESH)
    pl.semaphore_wait(barrier, len(places))


def remote(src, dst, send, recv, place):
    return pltpu.make_async_remote_copy(
        src_ref=src, dst_ref=dst, send_sem=send, recv_sem=recv, device_id={"dp": place}, device_id_type=MESH
    )


def turned(turn):
    return tuple((turn + p) % 3 for p in range(3))


def sum_into(dst, terms, rows):
    def body(i, _):
        at = pl.ds(pl.multiple_of(i * 16, 16), 16)
        total = terms[0][at, :].astype(F32)
        for term in terms[1:]:
            total = total + term[at, :].astype(F32)
        dst[at, :] = total.astype(BF16)
        return 0

    lax.fori_loop(0, rows // 16, body, 0)


STAGES = ((1, 3, 5, 7), (2, 6), (4,))


def finish_kernel(cuts, d_ready, hid, dh, a, dgu, *refs):
    outs, full, rest = refs[:4], (d_ready, *refs[4:7]), refs[7:]
    jobs = [(q, start, width, turned(k)) for q in range(4) for k, (start, width) in enumerate(cuts[q])]
    n = len(jobs)
    own, paired, first, second, third = (rest[k * n : (k + 1) * n] for k in range(5))
    load_sem, send_pair, recv_pair, send, recv, weight_sem = rest[5 * n :]
    me = lax.axis_index("dp")
    core = lax.rem(me, 2)
    partner = flip(me, 1)
    near = [flip(me, bit) for bit in BITS]
    meet([*near, partner])

    def load(j):
        q, start, width, _ = jobs[j]
        return pltpu.make_async_copy(full[q].at[:, core, :, pl.ds(start, width)], own[j], load_sem.at[j])

    def pair(j):
        q, start, width, _ = jobs[j]
        return remote(full[q].at[:, 1 - core, :, pl.ds(start, width)], paired[j], send_pair.at[j], recv_pair.at[j], partner)

    def at(j, mask):
        return lax.div(flips(me, jobs[j][3], mask), 2)

    def stage_of(mask):
        return 0 if mask & 1 else 1 if mask & 2 else 2

    def hop(j, mask):
        stage = stage_of(mask)
        dst = (first, second, third)[stage][j].at[mask >> (stage + 1)]
        return remote(own[j].at[at(j, mask)], dst, send.at[j, mask], recv.at[j, mask], near[jobs[j][3][stage]])

    def add(j, mask, stage):
        terms = [own[j].at[at(j, mask)], paired[j].at[at(j, mask)]]
        for s in range(stage):
            hop(j, mask + (1 << s)).wait_recv()
            terms.append((first, second, third)[s][j].at[mask >> (s + 1)])
        q, start, width, _ = jobs[j]
        sum_into(own[j].at[at(j, mask)] if mask else outs[q].at[:, pl.ds(start, width)], terms, own[j].shape[1])

    def begin(q):
        for j in range(3 * q, 3 * q + 3):
            pair(j).start()
            load(j).start()

    def go(q, stage):
        for j in range(3 * q, 3 * q + 3):
            if stage == 0:
                load(j).wait()
                pair(j).wait_recv()
            for mask in STAGES[stage] if stage < 3 else (0,):
                add(j, mask, stage)
                if mask:
                    hop(j, mask).start()

    def matmuls(events, grid, ins, out, rhs=None):
        def body(*tiles):
            step = pl.program_id(0) * grid[1] + pl.program_id(1)
            for when, what in events.items():

                @pl.when(step == when)
                def _(what=what):
                    go(*what)

            lhs, tile = tiles[0], tiles[-1]
            right = tiles[1] if rhs is None else rhs
            tile[...] = dot(lhs[...], right[...], (0, 0)).astype(BF16).reshape(tile.shape)

        specs = [pl.BlockSpec(block, index) for _, block, index in ins]
        pltpu.emit_pipeline(body, grid=grid, in_specs=specs, out_specs=[pl.BlockSpec(out[1], out[2])])(*[i[0] for i in ins], out[0])

    begin(0)

    def down(rhs):
        copy = pltpu.make_async_copy(dh, rhs, weight_sem)
        copy.start()
        copy.wait()
        t, p = hid.shape
        rows, columns = full[1].shape[2:]
        tp = 2 * 2 * rows
        matmuls({3: (0, 0)}, (p // tp, 1), [(hid, (t, tp), lambda i, j: (0, i))], (full[1], (2, 2, rows, columns), lambda i, j: (i, 0, 0, 0)), rhs)

    pl.run_scoped(down, pltpu.VMEM(dh.shape, BF16))
    begin(1)
    t, p = a.shape
    rows, columns = full[2].shape[2:]
    tp, tq = 4 * 2 * rows, 512
    grid = (p // tp, columns // tq)
    for q, events in ((2, {3: (0, 1), 6: (1, 0), 11: (0, 2)}), (3, {2: (0, 3), 4: (1, 1), 6: (2, 0), 11: (1, 2)})):
        matmuls(
            events,
            grid,
            [(a, (t, tp), lambda i, j: (0, i)), (dgu.at[q - 2], (t, tq), lambda i, j: (0, j))],
            (full[q], (4, 2, rows, tq), lambda i, j: (i, 0, 0, j)),
        )
        begin(q)
    for what in ((1, 3), (2, 1), (3, 0), (2, 2), (3, 1), (2, 3), (3, 2), (3, 3)):
        go(*what)
    for j in range(n):
        pair(j).wait_send()
        for mask in range(1, 8):
            hop(j, mask).wait_send()


def thirds(columns):
    cuts, left = [], columns // 128
    for k in (3, 2, 1):
        cuts.append((columns - left * 128, left // k * 128))
        left -= left // k
    return tuple(cuts)


def finish(ready, hid, dh, a, dgu, collective_id):
    shapes = [(ready.shape[0] // 16, ready.shape[1]), (hid.shape[1] // 16, dh.shape[1]), *[(a.shape[1] // 16, dgu.shape[2])] * 2]
    cuts = [thirds(columns) for _, columns in shapes]
    buffers = lambda n: [pltpu.VMEM((n, rows, width), BF16) for (rows, _), cut in zip(shapes, cuts) for _, width in cut]
    sems, one = pltpu.SemaphoreType.DMA((12, 8)), pltpu.SemaphoreType.DMA((12,))
    blocked = [(8, 2, *shape) for shape in shapes]
    return pl.pallas_call(
        functools.partial(finish_kernel, cuts),
        out_shape=[jax.ShapeDtypeStruct(shape, BF16) for shape in (*shapes, *blocked[1:])],
        in_specs=[IN_HBM] * 5,
        out_specs=[IN_VMEM] * 4 + [IN_HBM] * 3,
        scratch_shapes=[
            *buffers(8), *buffers(8), *buffers(4), *buffers(2), *buffers(1), one, one, one, sems, sems, pltpu.SemaphoreType.DMA
        ],
        compiler_params=pltpu.CompilerParams(collective_id=collective_id, has_side_effects=True, vmem_limit_bytes=67043328),
        cost_estimate=pl.CostEstimate(flops=5 * 10**10, bytes_accessed=10**8, transcendentals=0),
        name="finish",
    )(ready.reshape(blocked[0]), hid, dh, a, dgu)[:4]


def total_kernel(count, *refs):
    grads, (out_ref, part_ref, held, send, recv) = refs[:count], refs[count:]
    me = lax.axis_index("dp")
    others = []
    for k in range(1, 16):
        place = me
        for bit in (1, 2, 4, 8):
            if k & bit:
                place = flip(place, bit)
        others.append(place)
    sums = jnp.zeros((8, 128), F32)
    for grad in grads:
        rows, columns = grad.shape

        def body(i, sums, grad=grad, columns=columns):
            g = grad[pl.ds(pl.multiple_of(i * 16, 16), 16), :].astype(F32)
            g = g * g
            g = g[:8] + g[8:]
            tiles = [g[:, c : c + 128] for c in range(0, columns, 128)]
            while len(tiles) > 1:
                tiles = [sum(tiles[c : c + 2]) for c in range(0, len(tiles), 2)]
            return sums + tiles[0]

        sums = lax.fori_loop(0, rows // 16, body, sums)
    part_ref[...] = sums
    meet(others)
    copies = []
    for k, place in enumerate(others):
        copies.append(remote(part_ref, held.at[k], send.at[k], recv.at[k], place))
        copies[-1].start()
    for copy in copies:
        copy.wait_recv()
    slots = [part_ref[...]] + [held[k] for k in range(15)]
    while len(slots) > 1:
        slots = [slots[i] + slots[i + 1] for i in range(0, len(slots), 2)]
    out_ref[...] = jnp.zeros((8, 128), F32) + jnp.sum(slots[0])
    for copy in copies:
        copy.wait_send()


def total_of(grads, collective_id):
    return pl.pallas_call(
        functools.partial(total_kernel, len(grads)),
        out_shape=jax.ShapeDtypeStruct((8, 128), F32),
        in_specs=[IN_VMEM] * len(grads),
        out_specs=IN_VMEM,
        scratch_shapes=[
            pltpu.VMEM((8, 128), F32), pltpu.VMEM((15, 8, 128), F32), pltpu.SemaphoreType.DMA((15,)), pltpu.SemaphoreType.DMA((15,))
        ],
        compiler_params=pltpu.CompilerParams(collective_id=collective_id, has_side_effects=True),
        name="total",
    )(*grads)[0, 0]


def gather_kernel(count, layers, *refs):
    blocks, outs, rest = refs[:count], refs[count : 2 * count], refs[2 * count :]
    held, (local_sem, send, recv, send_pair, recv_pair) = rest[:count], rest[count:]
    me = lax.axis_index("dp")
    partner = flip(me, 1)
    near = [flip(me, bit) for bit in BITS]
    meet([*near, partner])
    jobs = [(i, l) for l in range(layers) for i in range(count)]

    def slot(i, l, mask):
        return held[i].at[l, mask - 1] if mask else blocks[i].at[l]

    def place_in(i, l, owner):
        rows = blocks[i].shape[1]
        return outs[i].at[l, pl.ds(pl.multiple_of(owner * rows, rows), rows), :]

    hops, pairs, locals_ = {}, {}, {}

    def hop(i, l, mask, stage):
        number = mask + (1 << stage)
        at = (l * count + i, number - 1)
        hops[i, l, number] = remote(slot(i, l, mask), slot(i, l, number), send.at[at], recv.at[at], near[turned(i)[stage]])
        hops[i, l, number].start()

    def hand_on(i, l, mask):
        owner = flips(me, turned(i), mask)
        at = (l * count + i, mask)
        pairs[i, l, mask] = remote(slot(i, l, mask), place_in(i, l, owner), send_pair.at[at], recv_pair.at[at], partner)
        pairs[i, l, mask].start()
        locals_[i, l, mask] = pltpu.make_async_copy(slot(i, l, mask), place_in(i, l, owner), local_sem.at[at])
        locals_[i, l, mask].start()

    for stage in range(3):
        for i, l in jobs:
            hop(i, l, 0, stage)
    for i, l in jobs:
        hand_on(i, l, 0)
    for mask in range(1, 8):
        for i, l in jobs:
            hops[i, l, mask].wait_recv()
            for stage in range(3):
                if mask < 1 << stage:
                    hop(i, l, mask, stage)
            hand_on(i, l, mask)
    for copy in pairs.values():
        copy.wait()
    for copy in hops.values():
        copy.wait_send()
    for copy in locals_.values():
        copy.wait()


def gather(blocks, collective_id):
    count, layers = len(blocks), blocks[0].shape[0]
    shapes = [b.shape[1:] for b in blocks]
    jobs = count * layers
    sent = sum(b.size for b in blocks) * 2 * 15
    return pl.pallas_call(
        functools.partial(gather_kernel, count, layers),
        out_shape=[jax.ShapeDtypeStruct((layers, 16 * r, c), BF16) for r, c in shapes],
        in_specs=[IN_VMEM] * count,
        out_specs=[IN_HBM] * count,
        scratch_shapes=[
            *[pltpu.VMEM((layers, 7, r, c), BF16) for r, c in shapes],
            pltpu.SemaphoreType.DMA((jobs, 8)),
            *[pltpu.SemaphoreType.DMA((jobs, 7))] * 2,
            *[pltpu.SemaphoreType.DMA((jobs, 8))] * 2,
        ],
        compiler_params=pltpu.CompilerParams(collective_id=collective_id, has_side_effects=True, vmem_limit_bytes=VMEM_BYTES),
        cost_estimate=pl.CostEstimate(flops=10**10, bytes_accessed=sent, transcendentals=0),
        name="gather",
    )(*blocks)


def dot(a, b, contract):
    return lax.dot_general(a, b, ((contract[:1], contract[1:]), ((), ())), preferred_element_type=F32)


def scale_of(wide):
    return lax.rsqrt(jnp.mean(wide * wide, -1, keepdims=True) + 1e-6)


def normed(h):
    wide = h.astype(F32)
    return (wide * scale_of(wide)).astype(BF16)


def gated_back(gate, up, d):
    s = jax.nn.sigmoid(gate)
    return (d * up * (s * (1 + gate * (1 - s)))).astype(BF16), (d * (gate * s)).astype(BF16)


def run(kernel, name, grid, ins, outs, flops):
    moved = sum(a.size * a.dtype.itemsize for a, _, _ in ins)
    return pl.pallas_call(
        kernel,
        grid=grid,
        in_specs=[pl.BlockSpec(block, index) for _, block, index in ins],
        out_specs=[pl.BlockSpec(block, index) for _, _, block, index in outs],
        out_shape=[jax.ShapeDtypeStruct(shape, kind) for shape, kind, _, _ in outs],
        compiler_params=pltpu.CompilerParams(dimension_semantics=("arbitrary",) * len(grid), vmem_limit_bytes=VMEM_BYTES),
        cost_estimate=pl.CostEstimate(flops=flops, bytes_accessed=moved, transcendentals=0),
        name=name,
    )(*[a for a, _, _ in ins])


def pieces(width, piece):
    return [pl.ds(at, piece) for at in range(0, width, piece)]


def up_kernel(x_ref, wg_ref, wu_ref, a_ref, gate_ref, up_ref, hid_ref):
    @pl.when(pl.program_id(1) == 0)
    def _():
        def body(i, _):
            at = pl.ds(pl.multiple_of(i * 128, 128), 128)
            a_ref[at, :] = normed(x_ref[at, :])
            return 0

        lax.fori_loop(0, x_ref.shape[0] // 128, body, 0)

    for at in pieces(gate_ref.shape[1], 256):
        gate, up = dot(a_ref[...], wg_ref[0, :, at], (1, 0)), dot(a_ref[...], wu_ref[0, :, at], (1, 0))
        gate_ref[:, at] = gate
        up_ref[:, at] = up
        hid_ref[:, at] = (gate * jax.nn.sigmoid(gate) * up).astype(BF16)


def up_layer(x, wg, wu, l):
    (t, d), f = x.shape, wg.shape[2]
    tm, tn = 1024, 512
    row, weight, tile = (lambda i, j: (i, 0)), (lambda i, j: (l, 0, j)), (lambda i, j: (i, j))
    return run(
        up_kernel, "up", (t // tm, f // tn),
        [(x, (tm, d), row), (wg, (1, d, tn), weight), (wu, (1, d, tn), weight)],
        [((t, d), BF16, (tm, d), row), *[((t, f), kind, (tm, tn), tile) for kind in (F32, F32, BF16)]],
        4 * t * d * f,
    )


def down_kernel(hid_ref, w_ref, x_ref, h_ref, a_ref):
    half = hid_ref.shape[0] // 2
    for at in (pl.ds(0, half), pl.ds(half, half)):
        h = x_ref[at, :] + dot(hid_ref[at, :], w_ref[0], (1, 0)).astype(BF16)
        h_ref[at, :] = h
        a_ref[at, :] = normed(h)


def down_layer(hid, wd, x, l):
    (t, f), d = hid.shape, wd.shape[2]
    tm = 512
    row = lambda i: (i, 0)
    return run(
        down_kernel, "down", (t // tm,),
        [(hid, (tm, f), row), (wd, (1, f, d), lambda i: (l, 0, 0)), (x, (tm, d), row)],
        [((t, d), BF16, (tm, d), row)] * 2,
        2 * t * d * f,
    )


def turn_kernel(a_ref, dy_ref, wg_ref, wu_ref, wd_ref, hid_ref, dgate_ref, dup_ref):
    for at in pieces(hid_ref.shape[1], 256):
        gate, up = dot(a_ref[...], wg_ref[0, :, at], (1, 0)), dot(a_ref[...], wu_ref[0, :, at], (1, 0))
        d = dot(dy_ref[...], wd_ref[0, at, :], (1, 1)).astype(BF16).astype(F32)
        hid_ref[:, at] = (gate * jax.nn.sigmoid(gate) * up).astype(BF16)
        dgate_ref[:, at], dup_ref[:, at] = gated_back(gate, up, d)


def turn_layer(a, dy, wg, wu, wd, l):
    (t, d), f = a.shape, wg.shape[2]
    tm, tn = 1024, 512
    row, weight, tile = (lambda i, j: (i, 0)), (lambda i, j: (l, 0, j)), (lambda i, j: (i, j))
    return run(
        turn_kernel, "turn", (t // tm, f // tn),
        [(a, (tm, d), row), (dy, (tm, d), row), *[(w, (1, d, tn), weight) for w in (wg, wu)], (wd, (1, tn, d), lambda i, j: (l, j, 0))],
        [((t, f), BF16, (tm, tn), tile)] * 3,
        6 * t * d * f,
    )


def back_kernel(dgate_ref, dup_ref, wg_ref, wu_ref, h_ref, dy_ref, dh_ref):
    da = dot(dgate_ref[...], wg_ref[0], (1, 1)).astype(BF16) + dot(dup_ref[...], wu_ref[0], (1, 1)).astype(BF16)
    da, wide = da.astype(F32), h_ref[...].astype(F32)
    scale = scale_of(wide)
    dwide = scale * da - wide * (scale * scale * scale * jnp.mean(da * wide, -1, keepdims=True))
    dh_ref[...] = dy_ref[...] + dwide.astype(BF16)


def back_layer(dgate, dup, wg, wu, h, dy, l):
    (t, f), d = dgate.shape, wg.shape[1]
    tm = 512
    row = lambda i: (i, 0)
    return run(
        back_kernel, "back", (t // tm,),
        [*[(g, (tm, f), row) for g in (dgate, dup)], *[(w, (1, d, f), lambda i: (l, 0, 0)) for w in (wg, wu)], (h, (tm, d), row), (dy, (tm, d), row)],
        [((t, d), BF16, (tm, d), row)],
        4 * t * d * f,
    )[0]


def hidden_kernel(dh_ref, wd_ref, gate_ref, up_ref, both_ref):
    for at in pieces(gate_ref.shape[1], 512):
        d = dot(dh_ref[...], wd_ref[0, at, :], (1, 1)).astype(BF16).astype(F32)
        both_ref[0, :, at], both_ref[1, :, at] = gated_back(gate_ref[:, at], up_ref[:, at], d)


def hidden_back(dh, wd, gate, up, l):
    (t, d), f = dh.shape, gate.shape[1]
    tm = 256
    row = lambda i: (i, 0)
    return run(
        hidden_kernel, "hidden", (t // tm,),
        [(dh, (tm, d), row), (wd, (1, f, d), lambda i: (l, 0, 0)), (gate, (tm, f), row), (up, (tm, f), row)],
        [((2, t, f), BF16, (2, tm, f), lambda i: (0, i, 0))],
        2 * t * d * f,
    )[0]


def weight_kernel(a_ref, b_ref, out_ref):
    out_ref[...] = dot(a_ref[...], b_ref[...], (0, 0)).astype(BF16)


def weight_grad(a, b):
    (t, p), q = a.shape, b.shape[1]
    tp, tq = (640, 1024) if p < q else (768, 1280)
    return run(
        weight_kernel, "weight", (p // tp, q // tq),
        [(a, (t, tp), lambda i, j: (0, i)), (b, (t, tq), lambda i, j: (0, j))],
        [((p, q), BF16, (tp, tq), lambda i, j: (i, j))],
        2 * t * p * q,
    )[0]


def adamw(w, m, v, g):
    m = 0.9 * m + 0.1 * g
    v = 0.95 * v + 0.05 * g * g
    step = m * lax.rsqrt(v + 1e-8) + 0.1 * w
    return (w - 0.02 * step).astype(BF16), m, v


def solution(mesh):
    n = mesh.shape["dp"]

    def step(x, dy, wg, wu, wd, *moments):
        x, dy = x[0], dy[0]
        spread = lambda g: lax.psum_scatter(g, "dp", scatter_dimension=0, tiled=True)
        a0, gate0, up0, hid0 = up_layer(x, wg, wu, 0)
        h1, a1 = down_layer(hid0, wd, x, 0)
        hid1, dgate1, dup1 = turn_layer(a1, dy, wg, wu, wd, 1)
        gd1 = spread(weight_grad(hid1, dy))
        gg1 = spread(weight_grad(a1, dgate1))
        gu1 = weight_grad(a1, dup1)
        dh = back_layer(dgate1, dup1, wg, wu, h1, dy, 1)
        dgu = hidden_back(dh, wd, gate0, up0, 0)
        gu1, gd0, gg0, gu0 = finish(gu1, hid0, dh, a0, dgu, 0)
        grads = ((gg0, gg1), (gu0, gu1), (gd0, gd1))
        total = total_of([g for pair in grads for g in pair], 1)
        count = wg.size + wu.size + wd.size
        factor = jnp.minimum(1.0, 0.5 * lax.rsqrt(total / count + 1e-30))
        me = lax.axis_index("dp")
        new_w, new_m, new_v = [], [], []
        for w, m, v, pair in zip((wg, wu, wd), moments[:3], moments[3:], grads):
            rows = w.shape[1] // n
            mine = lax.dynamic_slice_in_dim(w, me * rows, rows, 1)
            g = jnp.stack(pair).astype(F32) * factor
            for to, value in zip((new_w, new_m, new_v), adamw(mine.astype(F32), m, v, g)):
                to.append(value)
        new_w = gather(new_w, 2)
        return (*new_w, *new_m, *new_v)

    whole, rows = P(None, None, None), P(None, "dp", None)
    outs = (P("rep", None, None),) * 3 + (P("rep", "dp", None),) * 6
    return jax.shard_map(
        step, mesh=mesh, in_specs=(P(("rep", "dp"), None, None),) * 2 + (whole,) * 3 + (rows,) * 6, out_specs=outs, check_vma=False
    )
```

```python
import functools

import jax
import jax.numpy as jnp
from jax import lax
from jax.experimental import pallas as pl
from jax.experimental.pallas import tpu as pltpu
from jax.sharding import PartitionSpec as P

F32, BF16 = jnp.float32, jnp.bfloat16
MESH = pl.DeviceIdType.MESH
BITS = (8, 4, 2)
VMEM_BYTES = 60 * 1024 * 1024
IN_VMEM, IN_HBM = pl.BlockSpec(memory_space=pltpu.VMEM), pl.BlockSpec(memory_space=pl.ANY)


def flip(place, bit):
    return place + bit * (1 - 2 * lax.rem(lax.div(place, bit), 2))


def flips(place, axes, mask):
    for p, axis in enumerate(axes):
        if mask >> p & 1:
            place = flip(place, BITS[axis])
    return place


def meet(places):
    barrier = pltpu.get_barrier_semaphore()
    for place in places:
        pl.semaphore_signal(barrier, inc=1, device_id={"dp": place}, device_id_type=MESH)
    pl.semaphore_wait(barrier, len(places))


def remote(src, dst, send, recv, place):
    return pltpu.make_async_remote_copy(
        src_ref=src, dst_ref=dst, send_sem=send, recv_sem=recv, device_id={"dp": place}, device_id_type=MESH
    )


def turned(turn):
    return tuple((turn + p) % 3 for p in range(3))


def sum_into(dst, terms, rows):
    def body(i, _):
        at = pl.ds(pl.multiple_of(i * 16, 16), 16)
        total = terms[0][at, :].astype(F32)
        for term in terms[1:]:
            total = total + term[at, :].astype(F32)
        dst[at, :] = total.astype(BF16)
        return 0

    lax.fori_loop(0, rows // 16, body, 0)


STAGES = ((1, 3, 5, 7), (2, 6), (4,))


def finish_kernel(cuts, hid, dh, a, dgu, *refs):
    outs, full, rest = refs[:3], refs[3:6], refs[6:]
    jobs = [(q, start, width, turned(k)) for q in range(3) for k, (start, width) in enumerate(cuts[q])]
    n = len(jobs)
    own, paired, first, second, third = (rest[k * n : (k + 1) * n] for k in range(5))
    load_sem, send_pair, recv_pair, send, recv, weight_sem = rest[5 * n :]
    me = lax.axis_index("dp")
    core = lax.rem(me, 2)
    partner = flip(me, 1)
    near = [flip(me, bit) for bit in BITS]
    meet([*near, partner])

    def load(j):
        q, start, width, _ = jobs[j]
        return pltpu.make_async_copy(full[q].at[:, core, :, pl.ds(start, width)], own[j], load_sem.at[j])

    def pair(j):
        q, start, width, _ = jobs[j]
        return remote(full[q].at[:, 1 - core, :, pl.ds(start, width)], paired[j], send_pair.at[j], recv_pair.at[j], partner)

    def at(j, mask):
        return lax.div(flips(me, jobs[j][3], mask), 2)

    def stage_of(mask):
        return 0 if mask & 1 else 1 if mask & 2 else 2

    def hop(j, mask):
        stage = stage_of(mask)
        dst = (first, second, third)[stage][j].at[mask >> (stage + 1)]
        return remote(own[j].at[at(j, mask)], dst, send.at[j, mask], recv.at[j, mask], near[jobs[j][3][stage]])

    def add(j, mask, stage):
        terms = [own[j].at[at(j, mask)], paired[j].at[at(j, mask)]]
        for s in range(stage):
            hop(j, mask + (1 << s)).wait_recv()
            terms.append((first, second, third)[s][j].at[mask >> (s + 1)])
        q, start, width, _ = jobs[j]
        sum_into(own[j].at[at(j, mask)] if mask else outs[q].at[:, pl.ds(start, width)], terms, own[j].shape[1])

    def begin(q):
        for j in range(3 * q, 3 * q + 3):
            pair(j).start()
            load(j).start()

    def go(q, stage):
        for j in range(3 * q, 3 * q + 3):
            if stage == 0:
                load(j).wait()
                pair(j).wait_recv()
            for mask in STAGES[stage] if stage < 3 else (0,):
                add(j, mask, stage)
                if mask:
                    hop(j, mask).start()

    def matmuls(events, grid, ins, out, rhs=None):
        def body(*tiles):
            step = pl.program_id(0) * grid[1] + pl.program_id(1)
            for when, what in events.items():

                @pl.when(step == when)
                def _(what=what):
                    go(*what)

            lhs, tile = tiles[0], tiles[-1]
            right = tiles[1] if rhs is None else rhs
            tile[...] = dot(lhs[...], right[...], (0, 0)).astype(BF16).reshape(tile.shape)

        specs = [pl.BlockSpec(block, index) for _, block, index in ins]
        pltpu.emit_pipeline(body, grid=grid, in_specs=specs, out_specs=[pl.BlockSpec(out[1], out[2])])(*[i[0] for i in ins], out[0])

    def down(rhs):
        copy = pltpu.make_async_copy(dh, rhs, weight_sem)
        copy.start()
        copy.wait()
        t, p = hid.shape
        rows, columns = full[0].shape[2:]
        tp = 2 * 2 * rows
        matmuls({}, (p // tp, 1), [(hid, (t, tp), lambda i, j: (0, i))], (full[0], (2, 2, rows, columns), lambda i, j: (i, 0, 0, 0)), rhs)

    pl.run_scoped(down, pltpu.VMEM(dh.shape, BF16))
    begin(0)
    t, p = a.shape
    rows, columns = full[1].shape[2:]
    tp, tq = 4 * 2 * rows, 1024
    grid = (p // tp, columns // tq)
    for q, events in ((1, {3: (0, 0)}), (2, {2: (0, 1), 3: (1, 0), 5: (0, 2)})):
        matmuls(
            events,
            grid,
            [(a, (t, tp), lambda i, j: (0, i)), (dgu.at[q - 1], (t, tq), lambda i, j: (0, j))],
            (full[q], (4, 2, rows, tq), lambda i, j: (i, 0, 0, j)),
        )
        begin(q)
    for what in ((0, 3), (1, 1), (2, 0), (1, 2), (2, 1), (1, 3), (2, 2), (2, 3)):
        go(*what)
    for j in range(n):
        pair(j).wait_send()
        for mask in range(1, 8):
            hop(j, mask).wait_send()


def thirds(columns):
    cuts, left = [], columns // 128
    for k in (3, 2, 1):
        cuts.append((columns - left * 128, left // k * 128))
        left -= left // k
    return tuple(cuts)


def finish(hid, dh, a, dgu, collective_id):
    shapes = [(hid.shape[1] // 16, dh.shape[1]), *[(a.shape[1] // 16, dgu.shape[2])] * 2]
    cuts = [thirds(columns) for _, columns in shapes]
    buffers = lambda n: [pltpu.VMEM((n, rows, width), BF16) for (rows, _), cut in zip(shapes, cuts) for _, width in cut]
    sems, one = pltpu.SemaphoreType.DMA((9, 8)), pltpu.SemaphoreType.DMA((9,))
    blocked = [(8, 2, *shape) for shape in shapes]
    return pl.pallas_call(
        functools.partial(finish_kernel, cuts),
        out_shape=[jax.ShapeDtypeStruct(shape, BF16) for shape in (*shapes, *blocked)],
        in_specs=[IN_HBM] * 4,
        out_specs=[IN_VMEM] * 3 + [IN_HBM] * 3,
        scratch_shapes=[
            *buffers(8), *buffers(8), *buffers(4), *buffers(2), *buffers(1), one, one, one, sems, sems, pltpu.SemaphoreType.DMA
        ],
        compiler_params=pltpu.CompilerParams(collective_id=collective_id, has_side_effects=True, vmem_limit_bytes=67043328),
        cost_estimate=pl.CostEstimate(flops=5 * 10**10, bytes_accessed=10**8, transcendentals=0),
        name="finish",
    )(hid, dh, a, dgu)[:3]


def total_kernel(count, *refs):
    grads, (out_ref, part_ref, held, send, recv) = refs[:count], refs[count:]
    me = lax.axis_index("dp")
    others = []
    for k in range(1, 16):
        place = me
        for bit in (1, 2, 4, 8):
            if k & bit:
                place = flip(place, bit)
        others.append(place)
    sums = jnp.zeros((8, 128), F32)
    for grad in grads:
        rows, columns = grad.shape

        def body(i, sums, grad=grad, columns=columns):
            g = grad[pl.ds(pl.multiple_of(i * 16, 16), 16), :].astype(F32)
            g = g * g
            g = g[:8] + g[8:]
            tiles = [g[:, c : c + 128] for c in range(0, columns, 128)]
            while len(tiles) > 1:
                tiles = [sum(tiles[c : c + 2]) for c in range(0, len(tiles), 2)]
            return sums + tiles[0]

        sums = lax.fori_loop(0, rows // 16, body, sums)
    part_ref[...] = sums
    meet(others)
    copies = []
    for k, place in enumerate(others):
        copies.append(remote(part_ref, held.at[k], send.at[k], recv.at[k], place))
        copies[-1].start()
    for copy in copies:
        copy.wait_recv()
    slots = [part_ref[...]] + [held[k] for k in range(15)]
    while len(slots) > 1:
        slots = [slots[i] + slots[i + 1] for i in range(0, len(slots), 2)]
    out_ref[...] = jnp.zeros((8, 128), F32) + jnp.sum(slots[0])
    for copy in copies:
        copy.wait_send()


def total_of(grads, collective_id):
    return pl.pallas_call(
        functools.partial(total_kernel, len(grads)),
        out_shape=jax.ShapeDtypeStruct((8, 128), F32),
        in_specs=[IN_VMEM] * len(grads),
        out_specs=IN_VMEM,
        scratch_shapes=[
            pltpu.VMEM((8, 128), F32), pltpu.VMEM((15, 8, 128), F32), pltpu.SemaphoreType.DMA((15,)), pltpu.SemaphoreType.DMA((15,))
        ],
        compiler_params=pltpu.CompilerParams(collective_id=collective_id, has_side_effects=True),
        name="total",
    )(*grads)[0, 0]


def gather_kernel(count, layers, *refs):
    blocks, outs, rest = refs[:count], refs[count : 2 * count], refs[2 * count :]
    held, (local_sem, send, recv, send_pair, recv_pair) = rest[:count], rest[count:]
    me = lax.axis_index("dp")
    partner = flip(me, 1)
    near = [flip(me, bit) for bit in BITS]
    meet([*near, partner])
    jobs = [(i, l) for l in range(layers) for i in range(count)]

    def slot(i, l, mask):
        return held[i].at[l, mask - 1] if mask else blocks[i].at[l]

    def place_in(i, l, owner):
        rows = blocks[i].shape[1]
        return outs[i].at[l, pl.ds(pl.multiple_of(owner * rows, rows), rows), :]

    hops, pairs, locals_ = {}, {}, {}

    def hop(i, l, mask, stage):
        number = mask + (1 << stage)
        at = (l * count + i, number - 1)
        hops[i, l, number] = remote(slot(i, l, mask), slot(i, l, number), send.at[at], recv.at[at], near[turned(i)[stage]])
        hops[i, l, number].start()

    def hand_on(i, l, mask):
        owner = flips(me, turned(i), mask)
        at = (l * count + i, mask)
        pairs[i, l, mask] = remote(slot(i, l, mask), place_in(i, l, owner), send_pair.at[at], recv_pair.at[at], partner)
        pairs[i, l, mask].start()
        locals_[i, l, mask] = pltpu.make_async_copy(slot(i, l, mask), place_in(i, l, owner), local_sem.at[at])
        locals_[i, l, mask].start()

    for stage in range(3):
        for i, l in jobs:
            hop(i, l, 0, stage)
    for i, l in jobs:
        hand_on(i, l, 0)
    for mask in range(1, 8):
        for i, l in jobs:
            hops[i, l, mask].wait_recv()
            for stage in range(3):
                if mask < 1 << stage:
                    hop(i, l, mask, stage)
            hand_on(i, l, mask)
    for copy in pairs.values():
        copy.wait()
    for copy in hops.values():
        copy.wait_send()
    for copy in locals_.values():
        copy.wait()


def gather(blocks, collective_id):
    count, layers = len(blocks), blocks[0].shape[0]
    shapes = [b.shape[1:] for b in blocks]
    jobs = count * layers
    sent = sum(b.size for b in blocks) * 2 * 15
    return pl.pallas_call(
        functools.partial(gather_kernel, count, layers),
        out_shape=[jax.ShapeDtypeStruct((layers, 16 * r, c), BF16) for r, c in shapes],
        in_specs=[IN_VMEM] * count,
        out_specs=[IN_HBM] * count,
        scratch_shapes=[
            *[pltpu.VMEM((layers, 7, r, c), BF16) for r, c in shapes],
            pltpu.SemaphoreType.DMA((jobs, 8)),
            *[pltpu.SemaphoreType.DMA((jobs, 7))] * 2,
            *[pltpu.SemaphoreType.DMA((jobs, 8))] * 2,
        ],
        compiler_params=pltpu.CompilerParams(collective_id=collective_id, has_side_effects=True, vmem_limit_bytes=VMEM_BYTES),
        cost_estimate=pl.CostEstimate(flops=10**10, bytes_accessed=sent, transcendentals=0),
        name="gather",
    )(*blocks)


def dot(a, b, contract):
    return lax.dot_general(a, b, ((contract[:1], contract[1:]), ((), ())), preferred_element_type=F32)


def scale_of(wide):
    return lax.rsqrt(jnp.mean(wide * wide, -1, keepdims=True) + 1e-6)


def normed(h):
    wide = h.astype(F32)
    return (wide * scale_of(wide)).astype(BF16)


def gated_back(gate, up, d):
    s = jax.nn.sigmoid(gate)
    return (d * up * (s * (1 + gate * (1 - s)))).astype(BF16), (d * (gate * s)).astype(BF16)


def run(kernel, name, grid, ins, outs, flops):
    moved = sum(a.size * a.dtype.itemsize for a, _, _ in ins)
    return pl.pallas_call(
        kernel,
        grid=grid,
        in_specs=[pl.BlockSpec(block, index) for _, block, index in ins],
        out_specs=[pl.BlockSpec(block, index) for _, _, block, index in outs],
        out_shape=[jax.ShapeDtypeStruct(shape, kind) for shape, kind, _, _ in outs],
        compiler_params=pltpu.CompilerParams(dimension_semantics=("arbitrary",) * len(grid), vmem_limit_bytes=VMEM_BYTES),
        cost_estimate=pl.CostEstimate(flops=flops, bytes_accessed=moved, transcendentals=0),
        name=name,
    )(*[a for a, _, _ in ins])


def pieces(width, piece):
    return [pl.ds(at, piece) for at in range(0, width, piece)]


def up_kernel(x_ref, wg_ref, wu_ref, a_ref, gate_ref, up_ref, hid_ref):
    @pl.when(pl.program_id(1) == 0)
    def _():
        def body(i, _):
            at = pl.ds(pl.multiple_of(i * 128, 128), 128)
            a_ref[at, :] = normed(x_ref[at, :])
            return 0

        lax.fori_loop(0, x_ref.shape[0] // 128, body, 0)

    for at in pieces(gate_ref.shape[1], 256):
        gate, up = dot(a_ref[...], wg_ref[0, :, at], (1, 0)), dot(a_ref[...], wu_ref[0, :, at], (1, 0))
        gate_ref[:, at] = gate
        up_ref[:, at] = up
        hid_ref[:, at] = (gate * jax.nn.sigmoid(gate) * up).astype(BF16)


def up_layer(x, wg, wu, l):
    (t, d), f = x.shape, wg.shape[2]
    tm, tn = 1024, 512
    row, weight, tile = (lambda i, j: (i, 0)), (lambda i, j: (l, 0, j)), (lambda i, j: (i, j))
    return run(
        up_kernel, "up", (t // tm, f // tn),
        [(x, (tm, d), row), (wg, (1, d, tn), weight), (wu, (1, d, tn), weight)],
        [((t, d), BF16, (tm, d), row), *[((t, f), kind, (tm, tn), tile) for kind in (F32, F32, BF16)]],
        4 * t * d * f,
    )


def down_kernel(hid_ref, w_ref, x_ref, h_ref, a_ref):
    half = hid_ref.shape[0] // 2
    for at in (pl.ds(0, half), pl.ds(half, half)):
        h = x_ref[at, :] + dot(hid_ref[at, :], w_ref[0], (1, 0)).astype(BF16)
        h_ref[at, :] = h
        a_ref[at, :] = normed(h)


def down_layer(hid, wd, x, l):
    (t, f), d = hid.shape, wd.shape[2]
    tm = 512
    row = lambda i: (i, 0)
    return run(
        down_kernel, "down", (t // tm,),
        [(hid, (tm, f), row), (wd, (1, f, d), lambda i: (l, 0, 0)), (x, (tm, d), row)],
        [((t, d), BF16, (tm, d), row)] * 2,
        2 * t * d * f,
    )


def turn_kernel(a_ref, dy_ref, wg_ref, wu_ref, wd_ref, hid_ref, dgate_ref, dup_ref):
    for at in pieces(hid_ref.shape[1], 256):
        gate, up = dot(a_ref[...], wg_ref[0, :, at], (1, 0)), dot(a_ref[...], wu_ref[0, :, at], (1, 0))
        d = dot(dy_ref[...], wd_ref[0, at, :], (1, 1)).astype(BF16).astype(F32)
        hid_ref[:, at] = (gate * jax.nn.sigmoid(gate) * up).astype(BF16)
        dgate_ref[:, at], dup_ref[:, at] = gated_back(gate, up, d)


def turn_layer(a, dy, wg, wu, wd, l):
    (t, d), f = a.shape, wg.shape[2]
    tm, tn = 1024, 512
    row, weight, tile = (lambda i, j: (i, 0)), (lambda i, j: (l, 0, j)), (lambda i, j: (i, j))
    return run(
        turn_kernel, "turn", (t // tm, f // tn),
        [(a, (tm, d), row), (dy, (tm, d), row), *[(w, (1, d, tn), weight) for w in (wg, wu)], (wd, (1, tn, d), lambda i, j: (l, j, 0))],
        [((t, f), BF16, (tm, tn), tile)] * 3,
        6 * t * d * f,
    )


def back_kernel(dgate_ref, dup_ref, wg_ref, wu_ref, h_ref, dy_ref, dh_ref):
    da = dot(dgate_ref[...], wg_ref[0], (1, 1)).astype(BF16) + dot(dup_ref[...], wu_ref[0], (1, 1)).astype(BF16)
    da, wide = da.astype(F32), h_ref[...].astype(F32)
    scale = scale_of(wide)
    dwide = scale * da - wide * (scale * scale * scale * jnp.mean(da * wide, -1, keepdims=True))
    dh_ref[...] = dy_ref[...] + dwide.astype(BF16)


def back_layer(dgate, dup, wg, wu, h, dy, l):
    (t, f), d = dgate.shape, wg.shape[1]
    tm = 512
    row = lambda i: (i, 0)
    return run(
        back_kernel, "back", (t // tm,),
        [*[(g, (tm, f), row) for g in (dgate, dup)], *[(w, (1, d, f), lambda i: (l, 0, 0)) for w in (wg, wu)], (h, (tm, d), row), (dy, (tm, d), row)],
        [((t, d), BF16, (tm, d), row)],
        4 * t * d * f,
    )[0]


def hidden_kernel(dh_ref, wd_ref, gate_ref, up_ref, both_ref):
    for at in pieces(gate_ref.shape[1], 512):
        d = dot(dh_ref[...], wd_ref[0, at, :], (1, 1)).astype(BF16).astype(F32)
        both_ref[0, :, at], both_ref[1, :, at] = gated_back(gate_ref[:, at], up_ref[:, at], d)


def hidden_back(dh, wd, gate, up, l):
    (t, d), f = dh.shape, gate.shape[1]
    tm = 256
    row = lambda i: (i, 0)
    return run(
        hidden_kernel, "hidden", (t // tm,),
        [(dh, (tm, d), row), (wd, (1, f, d), lambda i: (l, 0, 0)), (gate, (tm, f), row), (up, (tm, f), row)],
        [((2, t, f), BF16, (2, tm, f), lambda i: (0, i, 0))],
        2 * t * d * f,
    )[0]


def weight_kernel(a_ref, b_ref, out_ref):
    out_ref[...] = dot(a_ref[...], b_ref[...], (0, 0)).astype(BF16)


def weight_grad(a, b):
    (t, p), q = a.shape, b.shape[1]
    tp, tq = (640, 1024) if p < q else (768, 1280)
    return run(
        weight_kernel, "weight", (p // tp, q // tq),
        [(a, (t, tp), lambda i, j: (0, i)), (b, (t, tq), lambda i, j: (0, j))],
        [((p, q), BF16, (tp, tq), lambda i, j: (i, j))],
        2 * t * p * q,
    )[0]


def adamw(w, m, v, g):
    m = 0.9 * m + 0.1 * g
    v = 0.95 * v + 0.05 * g * g
    step = m * lax.rsqrt(v + 1e-8) + 0.1 * w
    return (w - 0.02 * step).astype(BF16), m, v


def solution(mesh):
    n = mesh.shape["dp"]

    def step(x, dy, wg, wu, wd, *moments):
        x, dy = x[0], dy[0]
        spread = lambda g: lax.psum_scatter(g, "dp", scatter_dimension=0, tiled=True)
        a0, gate0, up0, hid0 = up_layer(x, wg, wu, 0)
        h1, a1 = down_layer(hid0, wd, x, 0)
        hid1, dgate1, dup1 = turn_layer(a1, dy, wg, wu, wd, 1)
        gd1 = spread(weight_grad(hid1, dy))
        gg1 = spread(weight_grad(a1, dgate1))
        gu1 = spread(weight_grad(a1, dup1))
        dh = back_layer(dgate1, dup1, wg, wu, h1, dy, 1)
        dgu = hidden_back(dh, wd, gate0, up0, 0)
        gd0, gg0, gu0 = finish(hid0, dh, a0, dgu, 0)
        grads = ((gg0, gg1), (gu0, gu1), (gd0, gd1))
        total = total_of([g for pair in grads for g in pair], 1)
        count = wg.size + wu.size + wd.size
        factor = jnp.minimum(1.0, 0.5 * lax.rsqrt(total / count + 1e-30))
        me = lax.axis_index("dp")
        new_w, new_m, new_v = [], [], []
        for w, m, v, pair in zip((wg, wu, wd), moments[:3], moments[3:], grads):
            rows = w.shape[1] // n
            mine = lax.dynamic_slice_in_dim(w, me * rows, rows, 1)
            g = jnp.stack(pair).astype(F32) * factor
            for to, value in zip((new_w, new_m, new_v), adamw(mine.astype(F32), m, v, g)):
                to.append(value)
        new_w = gather(new_w, 2)
        return (*new_w, *new_m, *new_v)

    whole, rows = P(None, None, None), P(None, "dp", None)
    outs = (P("rep", None, None),) * 3 + (P("rep", "dp", None),) * 6
    return jax.shard_map(
        step, mesh=mesh, in_specs=(P(("rep", "dp"), None, None),) * 2 + (whole,) * 3 + (rows,) * 6, out_specs=outs, check_vma=False
    )
```
